32 devices in a mesh: ba: 8 (over y, x, core), wa: 4 (over z).
Axes of the slice: x: 2, y: 2, z: 4, core: 2. Of those that a mesh axis runs over, the one named last changes fastest.
Arguments:
- sky_model: float32 [2, 2048, 2048], P(None, None, 'wa'), may hold values from -6 to 6
- plane_w: float32 [8], P('ba'), may hold values from -60 to 60
- kernel: float32 [16, 8], replicated, may hold values from -2 to 2
- tile_ids: int32 [512], P(('ba', 'wa')), may hold values from 0 to 255, as said below
- plane_ids: int32 [512, 1], P(('ba', 'wa')), may hold values from 0 to 7; in each aligned block of 16 rows (0 to 15, 16 to 31, ...) at most 2 rows name the same one
- positions: int32 [512, 2, 512], P(('ba', 'wa')), may hold values from 0 to 1935
- observed: float32 [512, 2, 512], P(('ba', 'wa')), may hold values from -6 to 6
Outputs:
- residual_vis: float32 [512, 2, 512], P(('ba', 'wa'))
The draws below stay inside these ranges and needn't reach their ends.
Inputs may be any that keep to these rules, and one draw needn't show every extreme that they name: `plane_ids`: among the 16 blocks of one device at most 2 name the same w-plane, and in every draw some device has a w-plane named by exactly 2 of its blocks. `tile_ids`: A tile id is row_tile * 16 + column_tile; the blocks held at index a of wa name column tiles a * 4 to (a + 1) * 4 - 1.
All inputs are finite; a program needn't handle non-finite values.
Results may differ from the reference program's by a relative error of at most 0.0003.
Values sent between devices are 32-bit elements; how exact they have to be, the bound alone decides.
A program may use at most 128 MiB of HBM per device.

```python
import math
import jax
import jax.numpy as jnp
import numpy as np
from jax import lax

N = 2048
TILE = 128
SUPPORT = 8
OVER = 16
SAMPLES = 512
BLK_DEV = 16
PLANES = 8
CAP = 2
NT = 16
NT_DEV = 4
BLOCKS = 512
N_BA = 8
N_WA = 4


def draw_tile_ids(key, part):
    row_key = jax.random.fold_in(key, 11)
    column_key = jax.random.fold_in(key, 12)
    row_tile = jax.random.randint(row_key, (BLOCKS,), 0, NT, dtype=jnp.int32)
    local_column = jax.random.randint(column_key, (BLOCKS,), 0, NT_DEV, dtype=jnp.int32)
    slab_index = jnp.arange(BLOCKS, dtype=jnp.int32) // BLK_DEV % N_WA
    return row_tile * NT + slab_index * NT_DEV + local_column


def with_ends(array, own_key, least, high):
    longest = array.shape.index(max(array.shape))
    spots = []
    for shift in (0, 1):
        where = [jax.random.randint(jax.random.fold_in(own_key, axis), (), 0, length) for axis, length in enumerate(array.shape)]
        where[longest] = (where[longest] + shift) % array.shape[longest]
        spots.append(tuple(where))
    return array.at[spots[0]].set(least).at[spots[1]].set(high)


def block_scale(stream_key, extent, pieces, low, largest):
    def one(dim, shards_of):
        steps = jax.random.uniform(jax.random.fold_in(jax.random.fold_in(stream_key, 6), dim), (shards_of,), jnp.float32, low / len(pieces), largest / len(pieces))
        return jnp.repeat(jnp.exp(steps), extent[dim] // shards_of).reshape((-1,) + (1,) * (len(extent) - dim - 1))

    level = one(*pieces[0])
    for cut in pieces[1:]:
        level = level * one(*cut)
    return level


def routed_block(own_key, own, number, rows, number_of, top, limit, lean):
    sequence = jax.random.permutation(own_key, number_of)
    heavy_load, ordinary = shares(number_of, rows * top, limit, lean, True), shares(number_of, rows * top, limit, lean, False)
    places = jnp.arange(number_of)

    def named(sizes, turn):
        used = int((sizes > 0).sum())
        fixed = max(1, used // 4)
        shifted = fixed + (places - fixed + turn * (used - fixed)) % max(1, number_of - fixed)
        return jnp.zeros((number_of,), jnp.int32).at[sequence[jnp.where(places < fixed, places, shifted)]].set(jnp.asarray(sizes, jnp.int32))

    sizes = jnp.where(number % 4 == 0, named(heavy_load, number // 4), named(ordinary, number - number // 4 - 1))
    mixed = jax.random.permutation(jax.random.fold_in(own, 3), number_of)
    source_of, taker = mixed[0:number_of // 2 * 2:2], mixed[1:number_of // 2 * 2:2]
    margin = jnp.minimum(sizes[source_of] - 1, limit - sizes[taker]) // 2
    margin = jnp.where((source_of == sequence[0]) | (taker == sequence[0]) | (sizes[taker] == 0), 0, jnp.maximum(margin, 0))
    shifted = jax.random.randint(jax.random.fold_in(own, 4), (number_of // 2,), 0, 1 << 20) % (margin + 1)
    sizes = sizes.at[source_of].add(-shifted).at[taker].add(shifted)
    items = jnp.searchsorted(jnp.cumsum(sizes), jnp.arange(rows * top), side="right").astype(jnp.int32)
    listing = items.reshape(top, rows).T
    listing = listing[jax.random.permutation(jax.random.fold_in(own, 1), rows)]
    turn = jax.random.randint(jax.random.fold_in(own, 2), (rows, 1), 0, top)
    return jnp.take_along_axis(listing, (jnp.arange(top)[None, :] + turn) % top, axis=1)


def shares(count, total, bound, lean, full):
    portions = [(1 << 20) // math.isqrt(rank ** lean) + 1 for rank in range(1, count + 1)]
    largest = bound if full else min(bound, max(-(-total // count), total * portions[0] // sum(portions)))
    least = 1 if total - largest >= count - 1 else 0
    holding, spare = [largest] + [least] * (count - 1), total - largest - least * (count - 1)
    while spare > 0:
        free = [i for i in range(1, count) if holding[i] < largest] or [i for i in range(1, count) if holding[i] < bound]
        pool, remaining = sum([portions[i] for i in free]), spare
        for i in free:
            extra = min(bound - holding[i], max(1, remaining * portions[i] // pool), spare)
            holding[i] = holding[i] + extra
            spare = spare - extra
    return np.array(holding)


def bell_draw(own_key, extent, spread, limit, split=(), held_as=jnp.bfloat16):
    factor_of = block_scale(own_key, extent, split, -0.22, 0.18) if split else 1.0
    values = jax.random.normal(own_key, extent, jnp.float32) * spread * factor_of
    return jnp.minimum(jnp.maximum(values, -limit), limit).astype(held_as)


def setup_inputs(seed: int = 0) -> dict:
    seeds = jax.random.split(jax.random.key(seed), 8)
    sky_model = bell_draw(seeds[0], (2, N, N), 1.0, 6.0, ((2, 4),), jnp.float32)
    plane_w = jnp.clip(jax.random.uniform(seeds[1], (PLANES,), jnp.float32, -60.0, 60.0) * block_scale(seeds[1], (PLANES,), ((0, 8),), -0.4, 0.0), -60.0, 60.0)
    kernel = bell_draw(seeds[2], (OVER, SUPPORT), 0.35, 2.0, (), jnp.float32)
    tile_ids = draw_tile_ids(jax.random.fold_in(seeds[7], 71), 0)
    plane_ids_keys = jax.random.split(jax.random.fold_in(seeds[4], 1), BLOCKS // BLK_DEV)
    plane_ids_turns = jax.random.permutation(jax.random.fold_in(seeds[4], 3), BLOCKS // BLK_DEV)
    plane_ids = jax.vmap(lambda own, number: routed_block(jax.random.fold_in(seeds[4], 2), own, number, BLK_DEV, PLANES, 1, CAP, 2))(plane_ids_keys, plane_ids_turns).reshape((BLOCKS, 1))
    positions = with_ends(jax.random.randint(seeds[5], (BLOCKS, 2, SAMPLES), 0, (TILE - SUPPORT + 1) * OVER), jax.random.fold_in(seeds[5], 1), 0, ((TILE - SUPPORT + 1) * OVER) - 1).astype(jnp.int32)
    observed = bell_draw(seeds[6], (BLOCKS, 2, SAMPLES), 1.0, 6.0, ((0, 32),), jnp.float32)
    return {"sky_model": sky_model, "plane_w": plane_w, "kernel": kernel, "tile_ids": tile_ids, "plane_ids": plane_ids, "positions": positions, "observed": observed}


FIELD_WIDTH = 0.7

def degrid_blocks(uv_grid, tile_list, fine_position, kernel):
    tiles_across = N // TILE
    row_tile = tile_list // tiles_across
    col_tile = tile_list % tiles_across
    cell_index = fine_position // OVER
    offset_index = fine_position % OVER
    kernel_taps = kernel[offset_index]
    tap_offsets = jnp.arange(SUPPORT, dtype=jnp.int32)
    row_cells = (row_tile * TILE)[:, None, None] + cell_index[:, 0, :, None] + tap_offsets
    col_cells = (col_tile * TILE)[:, None, None] + cell_index[:, 1, :, None] + tap_offsets
    patches = uv_grid[:, row_cells[:, :, :, None], col_cells[:, :, None, :]]
    return jnp.einsum('cmsij,msi,msj->mcs', patches, kernel_taps[:, 0], kernel_taps[:, 1])

def reference(sky_model, plane_w, kernel, tile_ids, plane_ids, positions, observed):
    coordinate = (jnp.arange(N, dtype=jnp.int32).astype(jnp.float32) - N / 2) * (FIELD_WIDTH / N)
    radius_sq = coordinate[:, None] ** 2 + coordinate[None, :] ** 2
    lowered = -radius_sq / (1.0 + jnp.sqrt(1.0 - radius_sq))
    target = plane_ids[:, 0]
    window = N_BA * N_WA * CAP
    sorted_blocks = jnp.argsort(target, stable=True).astype(jnp.int32)
    counts = lax.optimization_barrier(jnp.sum((target[None, :] == jnp.arange(PLANES, dtype=jnp.int32)[:, None]).astype(jnp.int32), axis=1))
    starts = (jnp.cumsum(counts) - counts).astype(jnp.int32)
    padded_order = jnp.concatenate([sorted_blocks, jnp.zeros((window,), jnp.int32)])

    def one_plane(predicted, plane_index):
        phase_angle = -2.0 * math.pi * plane_w[plane_index] * lowered
        cosine = jnp.cos(phase_angle)
        sine_part = jnp.sin(phase_angle)
        plane_image = lax.complex(sky_model[0] * cosine - sky_model[1] * sine_part, sky_model[0] * sine_part + sky_model[1] * cosine)
        spectrum = jnp.fft.fft2(plane_image).T / N
        uv_grid = jnp.stack([jnp.real(spectrum), jnp.imag(spectrum)])
        chosen = lax.dynamic_slice(padded_order, (starts[plane_index],), (window,))
        live_rows = jnp.arange(window, dtype=jnp.int32) < counts[plane_index]
        values_out = degrid_blocks(uv_grid, tile_ids[chosen], positions[chosen], kernel)
        predicted = predicted.at[chosen].add(jnp.where(live_rows[:, None, None], values_out, 0.0))
        return (predicted, None)
    predicted = lax.scan(one_plane, jnp.zeros(observed.shape, jnp.float32), jnp.arange(PLANES, dtype=jnp.int32))[0]
    return observed - predicted
```

```python
import functools
import math

import jax
import jax.numpy as jnp
import numpy as np
from jax import lax
from jax.experimental import pallas as pl
from jax.experimental.pallas import tpu as pltpu
from jax.sharding import PartitionSpec as P

TILE = 128
FIELD_WIDTH = 0.7


def halves(values):
    head = values.astype(jnp.bfloat16)
    rest = (values - head.astype(jnp.float32)).astype(jnp.bfloat16)
    return head, rest


def host_halves(values):
    values = values.astype(np.float32)
    head = values.astype(jnp.bfloat16)
    rest = (values - head.astype(np.float32)).astype(jnp.bfloat16)
    return head, rest


def roots(index, modulus):
    angle = -2.0 * np.pi * (index % modulus) / modulus
    return np.cos(angle), np.sin(angle)


def y_tables(extent):
    panels = extent // TILE
    residue = np.arange(panels, dtype=np.int64)[:, None, None]
    step = np.arange(TILE, dtype=np.int64)[None, :, None]
    row = np.arange(TILE, dtype=np.int64)[None, None, :]
    real, imag = roots((panels * step + residue) * row, extent)
    table = np.concatenate(
        [np.concatenate([real, -imag], axis=2), np.concatenate([imag, real], axis=2)], axis=1
    )
    return host_halves(table)


def x_tables(extent, columns):
    tiles = np.arange(extent // TILE, dtype=np.int64)[:, None, None]
    column = np.arange(columns, dtype=np.int64)[None, :, None]
    cell = np.arange(TILE, dtype=np.int64)[None, None, :]
    real, imag = roots((tiles * TILE + cell) * column, extent)
    return host_halves(np.concatenate([real, imag], axis=2))


def fit(function, top, terms):
    nodes = (np.cos((np.arange(400) + 0.5) * np.pi / 400) + 1.0) * 0.5 * top
    series = np.polynomial.chebyshev.Chebyshev.fit(nodes, function(nodes), terms - 1, domain=[0, top])
    return [float(c) for c in series.convert(kind=np.polynomial.Polynomial).coef]


def horner(coefficients, argument):
    total = coefficients[-1]
    for coefficient in coefficients[-2::-1]:
        total = total * argument + coefficient
    return total


def small_dft(values):
    count = len(values)
    if count == 1:
        return values
    even = small_dft(values[0::2])
    odd = small_dft(values[1::2])
    low, high = [], []
    for k in range(count // 2):
        real, imag = odd[k]
        if k == 0:
            pass
        elif 4 * k == count:
            real, imag = imag, -real
        elif 8 * k == count:
            h = math.sqrt(0.5)
            real, imag = (real + imag) * h, (imag - real) * h
        elif 8 * k == 3 * count:
            h = math.sqrt(0.5)
            real, imag = (imag - real) * h, (real + imag) * -h
        else:
            c = math.cos(-2.0 * math.pi * k / count)
            s = math.sin(-2.0 * math.pi * k / count)
            real, imag = real * c - imag * s, real * s + imag * c
        low.append((even[k][0] + real, even[k][1] + imag))
        high.append((even[k][0] - real, even[k][1] - imag))
    return low + high


def lane_lookup(table, index):
    numbers = lax.GatherDimensionNumbers(
        offset_dims=(),
        collapsed_slice_dims=(1,),
        start_index_map=(1,),
        operand_batching_dims=(0,),
        start_indices_batching_dims=(0,),
    )
    return lax.gather(
        table, index[..., None], numbers, (1, 1), mode=lax.GatherScatterMode.PROMISE_IN_BOUNDS
    )


def dot_exact(head_a, rest_a, head_b, rest_b):
    return jnp.dot(
        jnp.concatenate([head_a, head_a, rest_a], axis=1),
        jnp.concatenate([head_b, rest_b, head_b], axis=0),
        preferred_element_type=jnp.float32,
    )


def y_transform(extent, first, start, lanes, w, sky_ref, work):
    panels = extent // TILE
    spacing = FIELD_WIDTH / extent
    edge = 2.0 * (FIELD_WIDTH / 2) ** 2
    lower = fit(lambda r: 1.0 / (1.0 + np.sqrt(1.0 - r)), edge, 7)
    sine = fit(lambda z: np.sin(2 * np.pi * np.sqrt(z)) / np.sqrt(z), 0.25, 7)
    cosine = fit(lambda z: np.cos(2 * np.pi * np.sqrt(z)), 0.25, 7)

    for lane in range(0, lanes, 128):
        x = lax.broadcasted_iota(jnp.int32, (8, 128), 1) + (first + lane)
        x = (x.astype(jnp.float32) - extent / 2) * spacing
        x_sq = x * x

        @pl.loop(0, TILE // 8)
        def _(group):
            base = pl.multiple_of(group * 8, 8)
            row = (lax.broadcasted_iota(jnp.int32, (8, 128), 0) + base).astype(jnp.float32)
            values = []
            for panel in range(panels):
                y = (row + (panel * TILE - extent / 2)) * spacing
                radius = x_sq + y * y
                turns = radius * horner(lower, radius) * w
                turns = turns - jnp.round(turns)
                square = turns * turns
                s = turns * horner(sine, square)
                c = horner(cosine, square)
                real = sky_ref[0, pl.ds(base + panel * TILE, 8), pl.ds(start + lane, 128)]
                imag = sky_ref[1, pl.ds(base + panel * TILE, 8), pl.ds(start + lane, 128)]
                values.append((real * c - imag * s, real * s + imag * c))
            for residue, (real, imag) in enumerate(small_dft(values)):
                work[residue, pl.ds(base, 8), pl.ds(lane, 128)] = real
                work[residue, pl.ds(base + TILE, 8), pl.ds(lane, 128)] = imag


def y_finish(extent, start, work, table_head, table_rest, h_head, h_rest):
    panels = extent // TILE
    lanes = work.shape[2]
    per_tile = TILE // panels
    share = 8 // per_tile
    together = 16 // per_tile

    @pl.loop(0, panels // together)
    def _(step):
        products = []
        for i in range(together):
            residue = together * step + i
            head, rest = halves(work[residue])
            products.append(dot_exact(table_head[residue], table_rest[residue], head, rest))
        for part in range(2):
            rows = slice(part * TILE, (part + 1) * TILE)
            grouped = [product[rows].reshape(TILE // 8, 8, lanes) for product in products]
            at = pl.multiple_of(part * TILE + step * 16, 16)
            for place in range(share):
                cut = slice(place * per_tile, (place + 1) * per_tile)
                head, rest = halves(jnp.concatenate([group[:, cut] for group in grouped], axis=1))
                h_head[:, place, pl.ds(at, 16), pl.ds(start, lanes)] = head
                h_rest[:, place, pl.ds(at, 16), pl.ds(start, lanes)] = rest


def build_taps(taps_ref):
    over, support = taps_ref.shape
    lane = lax.broadcasted_iota(jnp.int32, (1, over * support), 1)
    table = jnp.zeros((1, over * support), jnp.float32)
    for o in range(over):
        for k in range(support):
            table = jnp.where(lane == k * over + (over - 1 - o), taps_ref[o, k], table)
    return table


def plane_kernel(
    extent, lanes, unroll,
    planes_ref, tiles_ref, w_ref, kernel_ref, pos_ref, sky_hbm, y_head, y_rest, e_head, e_rest,
    out_ref,
    sky, work, h_head, h_rest, yh, yr, eh, er, rows_head, rows_rest,
    send, asked, asked_tiles, values, answers, taps,
    local_sems, request_send, request_recv, answer_send, answer_recv, tile_sem,
):
    tiles_across = extent // TILE
    columns = eh.shape[1]
    share = h_head.shape[1]
    planes, slabs = lax.axis_size("ba"), lax.axis_size("wa")
    devices = planes * slabs
    plane, slab = lax.axis_index("ba"), lax.axis_index("wa")
    me = plane * slabs + slab
    blocks, _, samples = pos_ref.shape
    capacity = send.shape[1]
    over = kernel_ref.shape[0]

    chunks = columns // lanes
    loads = [
        pltpu.make_async_copy(
            sky_hbm.at[:, :, pl.ds(i * lanes, lanes)], sky.at[:, :, pl.ds(i * lanes, lanes)], local_sems.at[4 + i]
        )
        for i in range(chunks)
    ]
    copies = [
        pltpu.make_async_copy(source, target, local_sems.at[i])
        for i, (source, target) in enumerate(((y_head, yh), (y_rest, yr), (e_head, eh), (e_rest, er)))
    ]
    loads[0].start()
    copies[0].start()
    copies[1].start()
    for load in loads[1:]:
        load.start()
    copies[2].start()
    copies[3].start()

    def peer(offset):
        index = lax.rem(me + offset, devices)
        return index, {"ba": index // slabs, "wa": index % slabs}

    barrier = pltpu.get_barrier_semaphore()

    @pl.loop(1, devices)
    def _(offset):
        pl.semaphore_signal(
            barrier, inc=1, device_id=peer(offset)[1], device_id_type=pl.DeviceIdType.MESH
        )

    @pl.loop(0, planes)
    def _(p):
        count = jnp.int32(0)
        found = [jnp.int32(0)] * capacity
        for b in range(blocks):
            match = planes_ref[b, 0] == p
            for c in range(capacity):
                found[c] = jnp.where(match & (count == c), b, found[c])
            count = count + jnp.where(match, 1, 0)
        for c in range(capacity):
            b = found[c]
            for axis in range(2):
                send[p, c : c + 1, axis * samples : (axis + 1) * samples] = pos_ref[b, axis : axis + 1, :]
            send[p, c : c + 1, 2 * samples :] = jnp.full((1, 128), tiles_ref[b], jnp.int32)

    taps[...] = build_taps(kernel_ref)

    pl.semaphore_wait(barrier, devices - 1)

    def request(offset):
        index, where = peer(offset)
        return pltpu.make_async_remote_copy(
            src_ref=send.at[index // slabs],
            dst_ref=asked.at[me],
            send_sem=request_send.at[offset],
            recv_sem=request_recv.at[offset],
            device_id=where,
            device_id_type=pl.DeviceIdType.MESH,
        )

    @pl.loop(1, devices)
    def _(offset):
        request(offset).start()

    asked[me] = send[plane]

    for i in range(chunks):
        loads[i].wait()
        y_transform(extent, slab * columns + i * lanes, i * lanes, lanes, w_ref[0], sky, work)
        if i == 0:
            copies[0].wait()
            copies[1].wait()
        y_finish(extent, i * lanes, work, yh, yr, h_head, h_rest)

    copies[2].wait()
    copies[3].wait()

    @pl.loop(1, devices)
    def _(offset):
        request(offset).wait()

    tile_copy = pltpu.make_async_copy(asked.at[:, :, pl.ds(2 * samples, 128)], asked_tiles, tile_sem)
    tile_copy.start()
    tile_copy.wait()

    cell = lax.broadcasted_iota(jnp.int32, (1, TILE), 1)
    angle = ((cell * slab) % slabs).astype(jnp.float32) * (-2.0 * math.pi / slabs)
    turn_real = jnp.cos(angle) * (1.0 / extent)
    turn_imag = jnp.sin(angle) * (1.0 / extent)
    per = TILE // tiles_across

    def weights(axis, position):
        place = lax.broadcasted_iota(jnp.int32, (TILE, 128), 0)
        if axis == 1:
            place = (place % per) * tiles_across + place // per
        index = place * over + (over - 1) - position
        table = jnp.broadcast_to(taps[...], (TILE, 128))
        return jnp.where((index & -128) == 0, lane_lookup(table, index & 127), 0.0)

    def form_tile(tile):
        row_tile = tile // tiles_across
        col_tile = tile % tiles_across
        group, place = col_tile // share, col_tile % share
        both = dot_exact(h_head[group, place], h_rest[group, place], eh[row_tile], er[row_tile])
        real = both[:TILE, :TILE] - both[TILE:, TILE:]
        imag = both[:TILE, TILE:] + both[TILE:, :TILE]
        return halves(
            jnp.concatenate(
                [real * turn_real - imag * turn_imag, real * turn_imag + imag * turn_real], axis=0
            )
        )

    def row_weights(spot, owner, place):
        for lane in range(0, samples, 128):
            head, rest = halves(weights(0, asked[owner, place : place + 1, lane : lane + 128]))
            rows_head[spot, :, lane : lane + 128] = head
            rows_rest[spot, :, lane : lane + 128] = rest

    def predict(spot, owner, place, tile_pair):
        part = dot_exact(*tile_pair, rows_head[spot], rows_rest[spot])
        for lane in range(0, samples, 128):
            at = samples + lane
            column = weights(1, asked[owner, place : place + 1, at : at + 128])
            for c in range(2):
                outcome = part[c * TILE : (c + 1) * TILE, lane : lane + 128] * column
                at = c * samples + lane
                values[owner, place : place + 1, at : at + 128] = jnp.sum(outcome, axis=0, keepdims=True)

    def answer(offset):
        index, where = peer(offset)
        return pltpu.make_async_remote_copy(
            src_ref=values.at[index],
            dst_ref=answers.at[me],
            send_sem=answer_send.at[offset],
            recv_sem=answer_recv.at[offset],
            device_id=where,
            device_id_type=pl.DeviceIdType.MESH,
        )

    steps = devices // unroll

    @pl.loop(0, steps)
    def _(step):
        @pl.when(step > 0)
        def _():
            for o in range(unroll):
                answer((step - 1) * unroll + o + 1).start()

        work_list = [(peer(step * unroll + o + 1)[0], c) for o in range(unroll) for c in range(capacity)]
        tiles = [asked_tiles[owner, c, 0] for owner, c in work_list]
        pairs = {}
        for spot, (owner, c) in enumerate(work_list):
            row_weights(spot, owner, c)
            pairs[spot] = form_tile(tiles[spot])
            if spot:
                predict(spot - 1, *work_list[spot - 1], pairs.pop(spot - 1))
        predict(spot, *work_list[spot], pairs.pop(spot))

    for o in range(unroll - 1):
        answer((steps - 1) * unroll + o + 1).start()
    answers[me] = values[me]

    @pl.loop(1, devices)
    def _(offset):
        answer(offset).wait()

    @pl.loop(0, blocks)
    def _(b):
        p = planes_ref[b, 0]
        k = jnp.int32(0)
        for earlier in range(blocks):
            k = k + jnp.where((planes_ref[earlier, 0] == p) & (earlier < b), 1, 0)
        total = answers[p * slabs]
        for a in range(1, slabs):
            total += answers[p * slabs + a]
        own = total[0:1]
        for place in range(1, capacity):
            own = jnp.where(k == place, total[place : place + 1], own)
        for c in range(2):
            out_ref[b, c : c + 1, :] = own[:, c * samples : (c + 1) * samples]


def shards(sky_model, plane_w, kernel, tile_ids, plane_ids, positions, observed):
    extent, columns = sky_model.shape[1:]
    planes, slabs = lax.axis_size("ba"), lax.axis_size("wa")
    devices = planes * slabs
    block_count, _, samples = positions.shape
    tiles_across = extent // TILE
    capacity = max(2, block_count // planes)
    smem = pl.BlockSpec(memory_space=pltpu.SMEM)
    vmem = pl.BlockSpec(memory_space=pltpu.VMEM)
    hbm = pl.BlockSpec(memory_space=pl.ANY)
    length = 2 * samples + 128

    lanes = min(columns, 256)
    share = tiles_across * 8 // TILE
    unroll = math.gcd(devices, 4)
    over, support = kernel.shape
    y_head, y_rest = y_tables(extent)
    e_head, e_rest = x_tables(extent, columns)
    half = jnp.bfloat16
    dma = pltpu.SemaphoreType.DMA
    predicted = pl.pallas_call(
        functools.partial(plane_kernel, extent, lanes, unroll),
        in_specs=[smem, smem, smem, smem, vmem, hbm, hbm, hbm, hbm, hbm],
        out_specs=vmem,
        out_shape=jax.ShapeDtypeStruct(observed.shape, jnp.float32),
        scratch_shapes=[
            pltpu.VMEM((2, extent, columns), jnp.float32),
            pltpu.VMEM((tiles_across, 2 * TILE, lanes), jnp.float32),
            pltpu.VMEM((tiles_across // share, share, 2 * TILE, columns), half),
            pltpu.VMEM((tiles_across // share, share, 2 * TILE, columns), half),
            pltpu.VMEM(y_head.shape, half),
            pltpu.VMEM(y_head.shape, half),
            pltpu.VMEM(e_head.shape, half),
            pltpu.VMEM(e_head.shape, half),
            pltpu.VMEM((unroll * capacity, TILE, samples), half),
            pltpu.VMEM((unroll * capacity, TILE, samples), half),
            pltpu.VMEM((planes, capacity, length), jnp.int32),
            pltpu.VMEM((devices, capacity, length), jnp.int32),
            pltpu.SMEM((devices, capacity, 128), jnp.int32),
            pltpu.VMEM((devices, capacity, 2 * samples), jnp.float32),
            pltpu.VMEM((devices, capacity, 2 * samples), jnp.float32),
            pltpu.VMEM((1, over * support), jnp.float32),
            dma((4 + columns // lanes,)),
            dma((devices,)),
            dma((devices,)),
            dma((devices,)),
            dma((devices,)),
            dma,
        ],
        compiler_params=pltpu.CompilerParams(
            vmem_limit_bytes=60 << 20, collective_id=0, has_side_effects=True
        ),
        name="plane",
    )(
        plane_ids, tile_ids, plane_w, kernel, positions, sky_model,
        jnp.asarray(y_head), jnp.asarray(y_rest), jnp.asarray(e_head), jnp.asarray(e_rest),
    )
    return observed - predicted


def solution(mesh):
    return jax.shard_map(
        shards,
        mesh=mesh,
        in_specs=(
            P(None, None, "wa"),
            P("ba"),
            P(),
            P(("ba", "wa")),
            P(("ba", "wa"), None),
            P(("ba", "wa"), None, None),
            P(("ba", "wa"), None, None),
        ),
        out_specs=P(("ba", "wa"), None, None),
        check_vma=False,
    )
```

```python
import functools
import math

import jax
import jax.numpy as jnp
import numpy as np
from jax import lax
from jax.experimental import pallas as pl
from jax.experimental.pallas import tpu as pltpu
from jax.sharding import PartitionSpec as P

TILE = 128
FIELD_WIDTH = 0.7


def halves(values):
    head = values.astype(jnp.bfloat16)
    rest = (values - head.astype(jnp.float32)).astype(jnp.bfloat16)
    return head, rest


def host_halves(values):
    values = values.astype(np.float32)
    head = values.astype(jnp.bfloat16)
    rest = (values - head.astype(np.float32)).astype(jnp.bfloat16)
    return head, rest


def roots(index, modulus):
    angle = -2.0 * np.pi * (index % modulus) / modulus
    return np.cos(angle), np.sin(angle)


def y_tables(extent):
    panels = extent // TILE
    residue = np.arange(panels, dtype=np.int64)[:, None, None]
    step = np.arange(TILE, dtype=np.int64)[None, :, None]
    row = np.arange(TILE, dtype=np.int64)[None, None, :]
    real, imag = roots((panels * step + residue) * row, extent)
    table = np.concatenate(
        [np.concatenate([real, -imag], axis=2), np.concatenate([imag, real], axis=2)], axis=1
    )
    return host_halves(table)


def x_tables(extent, columns):
    tiles = np.arange(extent // TILE, dtype=np.int64)[:, None, None]
    pair = np.arange(columns // 2, dtype=np.int64)[None, :, None]
    cell = np.arange(TILE, dtype=np.int64)[None, None, :]
    real, imag = roots((tiles * TILE + cell) * (2 * pair + 1), 2 * extent)
    return np.concatenate(host_halves(np.concatenate([real, -imag], axis=1)), axis=2)


def fit(function, top, terms):
    nodes = (np.cos((np.arange(400) + 0.5) * np.pi / 400) + 1.0) * 0.5 * top
    series = np.polynomial.chebyshev.Chebyshev.fit(nodes, function(nodes), terms - 1, domain=[0, top])
    return [float(c) for c in series.convert(kind=np.polynomial.Polynomial).coef]


def horner(coefficients, argument):
    total = coefficients[-1]
    for coefficient in coefficients[-2::-1]:
        total = total * argument + coefficient
    return total


def small_dft(values):
    count = len(values)
    if count == 1:
        return values
    even = small_dft(values[0::2])
    odd = small_dft(values[1::2])
    low, high = [], []
    for k in range(count // 2):
        real, imag = odd[k]
        if k == 0:
            pass
        elif 4 * k == count:
            real, imag = imag, -real
        elif 8 * k == count:
            h = math.sqrt(0.5)
            real, imag = (real + imag) * h, (imag - real) * h
        elif 8 * k == 3 * count:
            h = math.sqrt(0.5)
            real, imag = (imag - real) * h, (real + imag) * -h
        else:
            c = math.cos(-2.0 * math.pi * k / count)
            s = math.sin(-2.0 * math.pi * k / count)
            real, imag = real * c - imag * s, real * s + imag * c
        low.append((even[k][0] + real, even[k][1] + imag))
        high.append((even[k][0] - real, even[k][1] - imag))
    return low + high


def lane_lookup(table, index):
    numbers = lax.GatherDimensionNumbers(
        offset_dims=(),
        collapsed_slice_dims=(1,),
        start_index_map=(1,),
        operand_batching_dims=(0,),
        start_indices_batching_dims=(0,),
    )
    return lax.gather(
        table, index[..., None], numbers, (1, 1), mode=lax.GatherScatterMode.PROMISE_IN_BOUNDS
    )


def dot_exact(head_a, rest_a, head_b, rest_b):
    return jnp.dot(
        jnp.concatenate([head_a, head_a, rest_a], axis=1),
        jnp.concatenate([head_b, rest_b, head_b], axis=0),
        preferred_element_type=jnp.float32,
    )


def interpolation(nodes):
    place = (np.arange(nodes) + 0.5) * np.pi / nodes
    at = np.arccos((np.arange(TILE) - (TILE - 1) / 2) / (TILE / 2))
    order = np.arange(nodes)
    scale = np.where(order == 0, 1.0, 2.0) / nodes
    head, rest = host_halves((np.cos(at[:, None] * order) * scale) @ np.cos(order[:, None] * place))
    return np.concatenate([head, head, rest], axis=1)


def y_phases(extent, first, stride, lanes, w, basis_ref, phases):
    panels = extent // TILE
    nodes = basis_ref.shape[1] // 3
    spacing = FIELD_WIDTH / extent
    edge = 2.0 * (FIELD_WIDTH / 2 * (1.0 + TILE / extent)) ** 2
    lower = fit(lambda r: 1.0 / (1.0 + np.sqrt(1.0 - r)), edge, 7)
    sine = fit(lambda z: np.sin(2 * np.pi * np.sqrt(z)) / np.sqrt(z), 0.25, 7)
    cosine = fit(lambda z: np.cos(2 * np.pi * np.sqrt(z)), 0.25, 7)
    x = lax.broadcasted_iota(jnp.int32, (nodes, lanes), 1) * stride + first
    x = (x.astype(jnp.float32) - extent / 2) * spacing
    x_sq = x * x
    node = lax.broadcasted_iota(jnp.int32, (nodes, 128), 0).astype(jnp.float32)
    node = jnp.cos((node + 0.5) * (math.pi / nodes)) * (TILE / 2) + (TILE - 1) / 2
    node = jnp.concatenate([node] * (lanes // 128), axis=1)
    basis = basis_ref[...]
    unroll = math.gcd(panels, 8)

    @pl.loop(0, panels // unroll)
    def _(step):
        for i in range(unroll):
            panel = step * unroll + i
            y = (node + ((panel * TILE).astype(jnp.float32) - extent / 2)) * spacing
            radius = x_sq + y * y
            turns = radius * horner(lower, radius) * w
            turns = turns - jnp.round(turns)
            square = turns * turns
            both = jnp.concatenate([horner(cosine, square), turns * horner(sine, square)], axis=1)
            head, rest = halves(both)
            phases[panel] = jnp.dot(
                basis, jnp.concatenate([head, rest, head], axis=0), preferred_element_type=jnp.float32
            )


def y_combine(extent, side, lanes, sky_ref, phases, work):
    panels = extent // TILE

    @pl.loop(0, TILE // 8)
    def _(group):
        base = pl.multiple_of(group * 8, 8)
        mirror = 127 - lax.broadcasted_iota(jnp.int32, (8, 128), 1)
        for lane in range(0, lanes, 128):
            at = lanes + lane if side else lanes - 128 - lane
            values = []
            for panel in range(panels):
                c = phases[panel, pl.ds(base, 8), pl.ds(lane, 128)]
                s = phases[panel, pl.ds(base, 8), pl.ds(lanes + lane, 128)]
                real, imag = (
                    sky_ref[part, pl.ds(base + panel * TILE, 8), pl.ds(at, 128)] for part in range(2)
                )
                if not side:
                    real, imag = lane_lookup(real, mirror), lane_lookup(imag, mirror)
                values.append((real * c - imag * s, real * s + imag * c))
            for residue, (real, imag) in enumerate(small_dft(values)):
                work[side, residue, pl.ds(base, 8), pl.ds(lane, 128)] = real
                work[side, residue, pl.ds(base + TILE, 8), pl.ds(lane, 128)] = imag


def y_finish(extent, work, table_head, table_rest, h_head, h_rest):
    panels = extent // TILE
    per_tile = TILE // panels
    share = 8 // per_tile
    together = 16 // per_tile
    unroll = math.gcd(panels // together, 4)

    @pl.loop(0, panels // together // unroll)
    def _(major):
        for minor in range(unroll):
            step = major * unroll + minor
            products = []
            for i in range(together):
                residue = together * step + i
                low, high = work[0, residue], work[1, residue]
                turned = jnp.concatenate([high[TILE:] - low[TILE:], low[:TILE] - high[:TILE]], axis=0)
                head, rest = halves(jnp.concatenate([low + high, turned], axis=1))
                products.append(dot_exact(table_head[residue], table_rest[residue], head, rest))
            for part in range(2):
                rows = slice(part * TILE, (part + 1) * TILE)
                grouped = [product[rows].reshape(TILE // 8, 8, -1) for product in products]
                at = pl.multiple_of(part * TILE + step * 16, 16)
                for place in range(share):
                    cut = slice(place * per_tile, (place + 1) * per_tile)
                    head, rest = halves(jnp.concatenate([group[:, cut] for group in grouped], axis=1))
                    h_head[:, place, pl.ds(at, 16), :] = head
                    h_rest[:, place, pl.ds(at, 16), :] = rest


def build_taps(taps_ref):
    support, over = taps_ref.shape
    lane = lax.broadcasted_iota(jnp.int32, (1, over * support), 1)
    table = jnp.zeros((1, over * support), jnp.float32)
    for o in range(over):
        for k in range(support):
            table = jnp.where(lane == k * over + (over - 1 - o), taps_ref[k, o], table)
    return table


def plane_kernel(
    extent, unroll,
    planes_ref, tiles_ref, w_ref, kernel_ref, pos_ref, sky_hbm, basis_ref, y_head, y_rest, e_both,
    out_ref,
    sky, phases, work, h_head, h_rest, yh, yr, eb, turns, rows_head, rows_rest, tile_head, tile_rest,
    send, asked, asked_tiles, values, answers, taps,
    local_sems, request_send, request_recv, answer_send, answer_recv, tile_sems,
):
    tiles_across = extent // TILE
    columns = sky.shape[2]
    lanes = columns // 2
    share = h_head.shape[1]
    planes, slabs = lax.axis_size("ba"), lax.axis_size("wa")
    devices = planes * slabs
    plane, slab = lax.axis_index("ba"), lax.axis_index("wa")
    me = plane * slabs + slab
    blocks, _, samples = pos_ref.shape
    capacity = send.shape[1]
    support, over = kernel_ref.shape
    per = TILE // tiles_across

    loads = [
        pltpu.make_async_copy(
            sky_hbm.at[:, :, pl.ds(i * lanes, lanes)], sky.at[:, :, pl.ds(i * lanes, lanes)], local_sems.at[i]
        )
        for i in range(2)
    ]
    copies = [
        pltpu.make_async_copy(source, target, local_sems.at[2 + i])
        for i, (source, target) in enumerate(((y_head, yh), (y_rest, yr), (e_both, eb)))
    ]
    for copy in loads + copies:
        copy.start()

    def peer(offset):
        index = lax.rem(me + offset, devices)
        return index, {"ba": index // slabs, "wa": index % slabs}

    barrier = pltpu.get_barrier_semaphore()

    @pl.loop(1, devices)
    def _(offset):
        pl.semaphore_signal(
            barrier, inc=1, device_id=peer(offset)[1], device_id_type=pl.DeviceIdType.MESH
        )

    @pl.loop(0, planes)
    def _(p):
        count = jnp.int32(0)
        found = [jnp.int32(0)] * capacity
        for b in range(blocks):
            match = planes_ref[0, b] == p
            for c in range(capacity):
                found[c] = jnp.where(match & (count == c), b, found[c])
            count = count + jnp.where(match, 1, 0)
        for c in range(capacity):
            b = found[c]
            for axis in range(2):
                send[p, c : c + 1, axis * samples : (axis + 1) * samples] = pos_ref[b, axis : axis + 1, :]
            send[p, c : c + 1, 2 * samples :] = jnp.full((1, 128), tiles_ref[b], jnp.int32)

    taps[...] = build_taps(kernel_ref)
    cell = lax.broadcasted_iota(jnp.int32, (tiles_across, TILE), 0) * TILE
    cell = cell + lax.broadcasted_iota(jnp.int32, (tiles_across, TILE), 1)
    angle = (cell * (2 * columns * slab + columns - 1)) % (2 * extent)
    angle = angle.astype(jnp.float32) * (-math.pi / extent)
    turns[0] = jnp.cos(angle) * (1.0 / extent)
    turns[1] = jnp.sin(angle) * (1.0 / extent)

    def request(offset):
        index, where = peer(offset)
        return pltpu.make_async_remote_copy(
            src_ref=send.at[index // slabs],
            dst_ref=asked.at[me],
            send_sem=request_send.at[offset],
            recv_sem=request_recv.at[offset],
            device_id=where,
            device_id_type=pl.DeviceIdType.MESH,
        )

    def tile_copy(offset):
        owner = peer(offset)[0]
        return pltpu.make_async_copy(
            asked.at[owner, :, pl.ds(2 * samples, 128)], asked_tiles.at[owner], tile_sems.at[offset - 1]
        )

    def receive(first):
        for o in range(unroll):
            offset = first + o

            @pl.when(offset < devices)
            def _():
                request(devices - offset).wait_recv()

            tile_copy(offset).start()

    first = slab * columns + lanes
    y_phases(extent, first - 1, -1, lanes, w_ref[0], basis_ref, phases)
    loads[0].wait()
    y_combine(extent, 0, lanes, sky, phases, work)
    pl.semaphore_wait(barrier, devices - 1)

    @pl.loop(1, devices)
    def _(i):
        request(devices - i).start()

    asked[me] = send[plane]
    rows_head[...] = jnp.zeros_like(rows_head)
    rows_rest[...] = jnp.zeros_like(rows_rest)
    tile_head[...] = jnp.zeros_like(tile_head)
    tile_rest[...] = jnp.zeros_like(tile_rest)
    y_phases(extent, first, 1, lanes, w_ref[0], basis_ref, phases)
    loads[1].wait()
    y_combine(extent, 1, lanes, sky, phases, work)
    copies[0].wait()
    copies[1].wait()
    receive(1)
    y_finish(extent, work, yh, yr, h_head, h_rest)
    copies[2].wait()

    row = lax.broadcasted_iota(jnp.int32, (8, 128), 0)
    table = jnp.broadcast_to(taps[...], (8, 128))

    def look_up(tap, position):
        return lane_lookup(table, ((tap * over) | ((over - 1) - (position & (over - 1)))) & 127)

    def form_tile(tile):
        row_tile = tile // tiles_across
        col_tile = tile % tiles_across
        group, place = col_tile // share, col_tile % share
        table = eb[row_tile]
        both = jnp.dot(
            jnp.concatenate([h_head[group, place], h_rest[group, place]], axis=1),
            jnp.concatenate([table, table], axis=0),
            preferred_element_type=jnp.float32,
        )
        both = both[:, :TILE] + both[:, TILE:]
        real, imag = both[:TILE], both[TILE:]
        turn_real, turn_imag = turns[0, pl.ds(row_tile, 1), :], turns[1, pl.ds(row_tile, 1), :]
        return halves(
            jnp.concatenate(
                [real * turn_real - imag * turn_imag, real * turn_imag + imag * turn_real], axis=0
            )
        )

    def row_weights(spot, owner, place):
        for lane in range(0, samples, 128):
            position = asked[owner, place : place + 1, lane : lane + 128]
            cell = position // over
            inner = cell & 7
            value = look_up((row - inner) & 7, position)
            at = (cell // 8) + jnp.where(row < inner, 1, 0)
            parts = [part.astype(jnp.float32) for part in halves(value)]
            for pair in range(0, TILE // 8, 2):
                hits = [at == pair, at == pair + 1]
                for part, target in zip(parts, (rows_head, rows_rest)):
                    target[spot, pair * 8 : pair * 8 + 16, lane : lane + 128] = jnp.concatenate(
                        [jnp.where(hit, part, 0.0) for hit in hits], axis=0
                    ).astype(target.dtype)

    def predict(spot, owner, place):
        slot = spot % 2
        part = dot_exact(tile_head[slot], tile_rest[slot], rows_head[spot], rows_rest[spot])
        for lane in range(0, samples, 128):
            at = samples + lane
            position = asked[owner, place : place + 1, at : at + 128]
            cell = position // over
            column = []
            for j in range(0, tiles_across, 8):
                tap = (row + j - cell) & (tiles_across - 1)
                column.append(jnp.where(tap < support, look_up(tap, position), 0.0))
            away = row * tiles_across - cell
            sums = [jnp.zeros((8, 128), jnp.float32)] * 2
            for j in range(tiles_across):
                hit = ((away + j) & -tiles_across) == 0
                weight = jnp.where(hit, column[j // 8][j % 8 : j % 8 + 1], 0.0)
                for c in range(2):
                    cut = c * TILE + j * per
                    sums[c] = sums[c] + part[cut : cut + per, lane : lane + 128] * weight
            for c in range(2):
                at = c * samples + lane
                values[owner, place : place + 1, at : at + 128] = jnp.sum(sums[c], axis=0, keepdims=True)

    def answer(offset):
        index, where = peer(offset)
        return pltpu.make_async_remote_copy(
            src_ref=values.at[index],
            dst_ref=answers.at[me],
            send_sem=answer_send.at[offset],
            recv_sem=answer_recv.at[offset],
            device_id=where,
            device_id_type=pl.DeviceIdType.MESH,
        )

    steps = devices // unroll
    work_list = [(o + 1, c) for o in range(unroll) for c in range(capacity)]

    @pl.loop(0, steps)
    def _(step):
        begin = step * unroll

        @pl.when(step < steps - 1)
        def _():
            receive(begin + unroll + 1)

        for o in range(unroll):
            tile_copy(begin + o + 1).wait()

        owners = [peer(begin + o)[0] for o in range(unroll + 1)]
        tiles = [asked_tiles[owners[o], c, 0] for o, c in work_list]
        last = len(work_list) - 1
        for spot, (o, c) in enumerate(work_list):
            row_weights(spot, owners[o], c)
            pair = form_tile(tiles[spot])
            if spot:
                predict(spot - 1, owners[work_list[spot - 1][0]], work_list[spot - 1][1])
            else:
                predict(last, owners[0], capacity - 1)
            tile_head[spot % 2], tile_rest[spot % 2] = pair

        @pl.when(step > 0)
        def _():
            answer(begin).start()

        for o in range(1, unroll):
            answer(begin + o).start()

    predict(len(work_list) - 1, me, capacity - 1)
    answers[me] = values[me]

    @pl.loop(1, devices)
    def _(offset):
        request(offset).wait_send()
        answer(offset).wait()

    @pl.loop(0, blocks)
    def _(b):
        p = planes_ref[0, b]
        k = jnp.int32(0)
        for earlier in range(blocks):
            k = k + jnp.where((planes_ref[0, earlier] == p) & (earlier < b), 1, 0)
        total = answers[p * slabs]
        for a in range(1, slabs):
            total += answers[p * slabs + a]
        own = total[0:1]
        for place in range(1, capacity):
            own = jnp.where(k == place, total[place : place + 1], own)
        for c in range(2):
            out_ref[b, c : c + 1, :] = own[:, c * samples : (c + 1) * samples]


def shards(sky_model, plane_w, kernel, tile_ids, plane_ids, positions, observed):
    extent, columns = sky_model.shape[1:]
    planes, slabs = lax.axis_size("ba"), lax.axis_size("wa")
    devices = planes * slabs
    block_count, _, samples = positions.shape
    tiles_across = extent // TILE
    capacity = max(2, block_count // planes)
    smem = pl.BlockSpec(memory_space=pltpu.SMEM)
    vmem = pl.BlockSpec(memory_space=pltpu.VMEM)
    hbm = pl.BlockSpec(memory_space=pl.ANY)
    length = 2 * samples + 128

    lanes = columns // 2
    share = tiles_across * 8 // TILE
    unroll = math.gcd(devices, 4)
    over, support = kernel.shape
    y_head, y_rest = y_tables(extent)
    e_both = x_tables(extent, columns)
    basis = jnp.asarray(interpolation(16))
    half = jnp.bfloat16
    dma = pltpu.SemaphoreType.DMA
    predicted = pl.pallas_call(
        functools.partial(plane_kernel, extent, unroll),
        in_specs=[smem, smem, smem, smem, vmem, hbm, vmem, hbm, hbm, hbm],
        out_specs=vmem,
        out_shape=jax.ShapeDtypeStruct(observed.shape, jnp.float32),
        scratch_shapes=[
            pltpu.VMEM((2, extent, columns), jnp.float32),
            pltpu.VMEM((tiles_across, TILE, 2 * lanes), jnp.float32),
            pltpu.VMEM((2, tiles_across, 2 * TILE, lanes), jnp.float32),
            pltpu.VMEM((tiles_across // share, share, 2 * TILE, columns), half),
            pltpu.VMEM((tiles_across // share, share, 2 * TILE, columns), half),
            pltpu.VMEM(y_head.shape, half),
            pltpu.VMEM(y_head.shape, half),
            pltpu.VMEM(e_both.shape, half),
            pltpu.VMEM((2, tiles_across, TILE), jnp.float32),
            pltpu.VMEM((unroll * capacity, TILE, samples), half),
            pltpu.VMEM((unroll * capacity, TILE, samples), half),
            pltpu.VMEM((2, 2 * TILE, TILE), half),
            pltpu.VMEM((2, 2 * TILE, TILE), half),
            pltpu.VMEM((planes, capacity, length), jnp.int32),
            pltpu.VMEM((devices, capacity, length), jnp.int32),
            pltpu.SMEM((devices, capacity, 128), jnp.int32),
            pltpu.VMEM((devices, capacity, 2 * samples), jnp.float32),
            pltpu.VMEM((devices, capacity, 2 * samples), jnp.float32),
            pltpu.VMEM((1, over * support), jnp.float32),
            dma((5,)),
            dma((devices,)),
            dma((devices,)),
            dma((devices,)),
            dma((devices,)),
            dma((devices,)),
        ],
        compiler_params=pltpu.CompilerParams(
            vmem_limit_bytes=60 << 20, collective_id=0, has_side_effects=True
        ),
        name="plane",
    )(
        plane_ids.T, tile_ids, plane_w, kernel.T, positions, sky_model, basis,
        jnp.asarray(y_head), jnp.asarray(y_rest), jnp.asarray(e_both),
    )
    return observed - predicted


def solution(mesh):
    return jax.shard_map(
        shards,
        mesh=mesh,
        in_specs=(
            P(None, None, "wa"),
            P("ba"),
            P(),
            P(("ba", "wa")),
            P(("ba", "wa"), None),
            P(("ba", "wa"), None, None),
            P(("ba", "wa"), None, None),
        ),
        out_specs=P(("ba", "wa"), None, None),
        check_vma=False,
    )
```

```python
import functools
import math

import jax
import jax.numpy as jnp
import numpy as np
from jax import lax
from jax.experimental import pallas as pl
from jax.experimental.pallas import tpu as pltpu
from jax.sharding import PartitionSpec as P

TILE = 128
FIELD_WIDTH = 0.7


def halves(values):
    head = values.astype(jnp.bfloat16)
    rest = (values - head.astype(jnp.float32)).astype(jnp.bfloat16)
    return head, rest


def host_halves(values):
    values = values.astype(np.float32)
    head = values.astype(jnp.bfloat16)
    rest = (values - head.astype(np.float32)).astype(jnp.bfloat16)
    return head, rest


def roots(index, modulus):
    angle = -2.0 * np.pi * (index % modulus) / modulus
    return np.cos(angle), np.sin(angle)


def y_tables(extent):
    panels = extent // TILE
    residue = np.arange(panels, dtype=np.int64)[:, None, None]
    step = np.arange(TILE, dtype=np.int64)[None, :, None]
    row = np.arange(TILE, dtype=np.int64)[None, None, :]
    real, imag = roots((panels * step + residue) * row, extent)
    table = np.concatenate(
        [np.concatenate([real, -imag], axis=2), np.concatenate([imag, real], axis=2)], axis=1
    )
    return host_halves(table)


def x_tables(extent, columns):
    tiles = np.arange(extent // TILE, dtype=np.int64)[:, None, None]
    pair = np.arange(columns // 2, dtype=np.int64)[None, :, None]
    cell = np.arange(TILE, dtype=np.int64)[None, None, :]
    real, imag = roots((tiles * TILE + cell) * (2 * pair + 1), 2 * extent)
    return np.concatenate(host_halves(np.concatenate([real, -imag], axis=1)), axis=2)


def fit(function, top, terms):
    nodes = (np.cos((np.arange(400) + 0.5) * np.pi / 400) + 1.0) * 0.5 * top
    series = np.polynomial.chebyshev.Chebyshev.fit(nodes, function(nodes), terms - 1, domain=[0, top])
    return [float(c) for c in series.convert(kind=np.polynomial.Polynomial).coef]


def horner(coefficients, argument):
    total = coefficients[-1]
    for coefficient in coefficients[-2::-1]:
        total = total * argument + coefficient
    return total


def small_dft(values):
    count = len(values)
    if count == 1:
        return [values[0]()]
    even = small_dft(values[0::2])
    odd = small_dft(values[1::2])
    low, high = [], []
    for k in range(count // 2):
        real, imag = odd[k]
        if k == 0:
            pass
        elif 4 * k == count:
            real, imag = imag, -real
        elif 8 * k == count:
            h = math.sqrt(0.5)
            real, imag = (real + imag) * h, (imag - real) * h
        elif 8 * k == 3 * count:
            h = math.sqrt(0.5)
            real, imag = (imag - real) * h, (real + imag) * -h
        else:
            c = math.cos(-2.0 * math.pi * k / count)
            s = math.sin(-2.0 * math.pi * k / count)
            real, imag = real * c - imag * s, real * s + imag * c
        low.append((even[k][0] + real, even[k][1] + imag))
        high.append((even[k][0] - real, even[k][1] - imag))
    return low + high


def lane_lookup(table, index):
    numbers = lax.GatherDimensionNumbers(
        offset_dims=(),
        collapsed_slice_dims=(1,),
        start_index_map=(1,),
        operand_batching_dims=(0,),
        start_indices_batching_dims=(0,),
    )
    return lax.gather(
        table, index[..., None], numbers, (1, 1), mode=lax.GatherScatterMode.PROMISE_IN_BOUNDS
    )


def dot_exact(head_a, rest_a, head_b, rest_b):
    return jnp.dot(
        jnp.concatenate([head_a, head_a, rest_a], axis=1),
        jnp.concatenate([head_b, rest_b, head_b], axis=0),
        preferred_element_type=jnp.float32,
    )


def interpolation(nodes):
    place = (np.arange(nodes) + 0.5) * np.pi / nodes
    at = np.arccos((np.arange(TILE) - (TILE - 1) / 2) / (TILE / 2))
    order = np.arange(nodes)
    scale = np.where(order == 0, 1.0, 2.0) / nodes
    head, rest = host_halves((np.cos(at[:, None] * order) * scale) @ np.cos(order[:, None] * place))
    return np.concatenate([head, head, rest], axis=1)


def y_phases(extent, first, stride, lanes, w, basis_ref, phases):
    panels = extent // TILE
    nodes = basis_ref.shape[1] // 3
    spacing = FIELD_WIDTH / extent
    edge = 2.0 * (FIELD_WIDTH / 2 * (1.0 + TILE / extent)) ** 2
    lower = fit(lambda r: 1.0 / (1.0 + np.sqrt(1.0 - r)), edge, 7)
    sine = fit(lambda z: np.sin(2 * np.pi * np.sqrt(z)) / np.sqrt(z), 0.25, 7)
    cosine = fit(lambda z: np.cos(2 * np.pi * np.sqrt(z)), 0.25, 7)
    x = lax.broadcasted_iota(jnp.int32, (nodes, lanes), 1) * stride + first
    x = (x.astype(jnp.float32) - extent / 2) * spacing
    x_sq = x * x
    node = lax.broadcasted_iota(jnp.int32, (nodes, 128), 0).astype(jnp.float32)
    node = jnp.cos((node + 0.5) * (math.pi / nodes)) * (TILE / 2) + (TILE - 1) / 2
    node = jnp.concatenate([node] * (lanes // 128), axis=1)
    basis = basis_ref[...]
    unroll = math.gcd(panels, 8)

    @pl.loop(0, panels // unroll)
    def _(step):
        for i in range(unroll):
            panel = step * unroll + i
            y = (node + ((panel * TILE).astype(jnp.float32) - extent / 2)) * spacing
            radius = x_sq + y * y
            turns = radius * horner(lower, radius) * w
            turns = turns - jnp.round(turns)
            square = turns * turns
            both = jnp.concatenate([horner(cosine, square), turns * horner(sine, square)], axis=1)
            head, rest = halves(both)
            phases[panel] = jnp.dot(
                basis, jnp.concatenate([head, rest, head], axis=0), preferred_element_type=jnp.float32
            )


def y_combine(extent, side, lanes, sky_ref, phases, work):
    panels = extent // TILE

    @pl.loop(0, TILE // 8, unroll=4)
    def _(group):
        base = pl.multiple_of(group * 8, 8)
        mirror = 127 - lax.broadcasted_iota(jnp.int32, (8, 128), 1)
        for lane in range(0, lanes, 128):
            at = lanes + lane if side else lanes - 128 - lane

            def value(panel):
                c = phases[panel, pl.ds(base, 8), pl.ds(lane, 128)]
                s = phases[panel, pl.ds(base, 8), pl.ds(lanes + lane, 128)]
                real, imag = (
                    sky_ref[part, pl.ds(base + panel * TILE, 8), pl.ds(at, 128)] for part in range(2)
                )
                if not side:
                    real, imag = lane_lookup(real, mirror), lane_lookup(imag, mirror)
                return real * c - imag * s, real * s + imag * c

            values = [functools.partial(value, panel) for panel in range(panels)]
            for residue, (real, imag) in enumerate(small_dft(values)):
                work[side, residue, pl.ds(base, 8), pl.ds(lane, 128)] = real
                work[side, residue, pl.ds(base + TILE, 8), pl.ds(lane, 128)] = imag


def y_finish(extent, work, table_head, table_rest, h_head, h_rest):
    panels = extent // TILE
    per_tile = TILE // panels
    share = 8 // per_tile
    together = 16 // per_tile
    unroll = math.gcd(panels // together, 4)

    @pl.loop(0, panels // together // unroll)
    def _(major):
        for minor in range(unroll):
            step = major * unroll + minor
            products = []
            for i in range(together):
                residue = together * step + i
                low, high = work[0, residue], work[1, residue]
                turned = jnp.concatenate([high[TILE:] - low[TILE:], low[:TILE] - high[:TILE]], axis=0)
                head, rest = halves(jnp.concatenate([low + high, turned], axis=1))
                products.append(dot_exact(table_head[residue], table_rest[residue], head, rest))
            for part in range(2):
                rows = slice(part * TILE, (part + 1) * TILE)
                grouped = [product[rows].reshape(TILE // 8, 8, -1) for product in products]
                at = pl.multiple_of(part * TILE + step * 16, 16)
                for place in range(share):
                    cut = slice(place * per_tile, (place + 1) * per_tile)
                    head, rest = halves(jnp.concatenate([group[:, cut] for group in grouped], axis=1))
                    h_head[:, place, pl.ds(at, 16), :] = head
                    h_rest[:, place, pl.ds(at, 16), :] = rest


def build_taps(taps_ref):
    support, over = taps_ref.shape
    lane = lax.broadcasted_iota(jnp.int32, (1, over * support), 1)
    table = jnp.zeros((1, over * support), jnp.float32)
    for o in range(over):
        for k in range(support):
            table = jnp.where(lane == k * over + (over - 1 - o), taps_ref[k, o], table)
    return table


def plane_kernel(
    extent, unroll,
    planes_hbm, tiles_hbm, w_ref, kernel_hbm, pos_hbm, sky_hbm, basis_hbm, y_head, y_rest, e_both,
    out_ref,
    planes_ref, tiles_ref, kernel_ref, pos_ref, basis_ref,
    sky, phases, work, h_head, h_rest, yh, yr, eb, turns, rows_head, rows_rest, tile_head, tile_rest,
    send, asked, asked_tiles, values, answers, taps,
    local_sems, request_send, request_recv, answer_send, answer_recv, tile_sems,
):
    tiles_across = extent // TILE
    columns = sky.shape[2]
    lanes = columns // 2
    share = h_head.shape[1]
    planes, slabs = lax.axis_size("ba"), lax.axis_size("wa")
    devices = planes * slabs
    plane, slab = lax.axis_index("ba"), lax.axis_index("wa")
    me = plane * slabs + slab
    blocks, _, samples = pos_ref.shape
    capacity = send.shape[1]
    support, over = kernel_ref.shape
    per = TILE // tiles_across

    loads = [
        pltpu.make_async_copy(
            sky_hbm.at[:, :, pl.ds(i * lanes, lanes)], sky.at[:, :, pl.ds(i * lanes, lanes)], local_sems.at[i]
        )
        for i in range(2)
    ]
    copies = [
        pltpu.make_async_copy(source, target, local_sems.at[2 + i])
        for i, (source, target) in enumerate(((y_head, yh), (y_rest, yr), (e_both, eb)))
    ]
    small = [
        pltpu.make_async_copy(source, target, local_sems.at[5 + i])
        for i, (source, target) in enumerate(
            (
                (basis_hbm, basis_ref), (planes_hbm, planes_ref), (tiles_hbm, tiles_ref),
                (kernel_hbm, kernel_ref), (pos_hbm, pos_ref),
            )
        )
    ]
    for copy in small + loads + copies:
        copy.start()

    def peer(offset):
        index = lax.rem(me + offset, devices)
        return index, {"ba": index // slabs, "wa": index % slabs}

    barrier = pltpu.get_barrier_semaphore()

    @pl.loop(1, devices)
    def _(offset):
        pl.semaphore_signal(
            barrier, inc=1, device_id=peer(offset)[1], device_id_type=pl.DeviceIdType.MESH
        )

    first = slab * columns + lanes
    small[0].wait()
    y_phases(extent, first - 1, -1, lanes, w_ref[0], basis_ref, phases)
    for copy in small[1:]:
        copy.wait()

    @pl.loop(0, planes)
    def _(p):
        count = jnp.int32(0)
        found = [jnp.int32(0)] * capacity
        for b in range(blocks):
            match = planes_ref[0, b] == p
            for c in range(capacity):
                found[c] = jnp.where(match & (count == c), b, found[c])
            count = count + jnp.where(match, 1, 0)
        for c in range(capacity):
            b = found[c]
            for axis in range(2):
                send[p, c : c + 1, axis * samples : (axis + 1) * samples] = pos_ref[b, axis : axis + 1, :]
            send[p, c : c + 1, 2 * samples :] = jnp.full((1, 128), tiles_ref[b], jnp.int32)

    taps[...] = build_taps(kernel_ref)
    cell = lax.broadcasted_iota(jnp.int32, (tiles_across, TILE), 0) * TILE
    cell = cell + lax.broadcasted_iota(jnp.int32, (tiles_across, TILE), 1)
    angle = (cell * (2 * columns * slab + columns - 1)) % (2 * extent)
    angle = angle.astype(jnp.float32) * (-math.pi / extent)
    turns[0] = jnp.cos(angle) * (1.0 / extent)
    turns[1] = jnp.sin(angle) * (1.0 / extent)

    def request(offset):
        index, where = peer(offset)
        return pltpu.make_async_remote_copy(
            src_ref=send.at[index // slabs],
            dst_ref=asked.at[me],
            send_sem=request_send.at[offset],
            recv_sem=request_recv.at[offset],
            device_id=where,
            device_id_type=pl.DeviceIdType.MESH,
        )

    def tile_copy(offset):
        owner = peer(offset)[0]
        return pltpu.make_async_copy(
            asked.at[owner, :, pl.ds(2 * samples, 128)], asked_tiles.at[owner], tile_sems.at[offset - 1]
        )

    def receive(first):
        for o in range(unroll):
            offset = first + o

            @pl.when(offset < devices)
            def _():
                request(devices - offset).wait_recv()

            tile_copy(offset).start()

    loads[0].wait()
    y_combine(extent, 0, lanes, sky, phases, work)
    pl.semaphore_wait(barrier, devices - 1)

    @pl.loop(1, devices)
    def _(i):
        request(devices - i).start()

    asked[me] = send[plane]
    last = rows_head.shape[0] - 1
    rows_head[last] = jnp.zeros(rows_head.shape[1:], rows_head.dtype)
    rows_rest[last] = jnp.zeros(rows_rest.shape[1:], rows_rest.dtype)
    tile_head[1] = jnp.zeros(tile_head.shape[1:], tile_head.dtype)
    tile_rest[1] = jnp.zeros(tile_rest.shape[1:], tile_rest.dtype)
    y_phases(extent, first, 1, lanes, w_ref[0], basis_ref, phases)
    loads[1].wait()
    y_combine(extent, 1, lanes, sky, phases, work)
    copies[0].wait()
    copies[1].wait()
    receive(1)
    y_finish(extent, work, yh, yr, h_head, h_rest)
    copies[2].wait()

    row = lax.broadcasted_iota(jnp.int32, (8, 128), 0)
    table = jnp.broadcast_to(taps[...], (8, 128))

    def look_up(tap, position):
        return lane_lookup(table, ((tap * over) | ((over - 1) - (position & (over - 1)))) & 127)

    def form_tile(tile):
        row_tile = tile // tiles_across
        col_tile = tile % tiles_across
        group, place = col_tile // share, col_tile % share
        table = eb[row_tile]
        both = jnp.dot(
            jnp.concatenate([h_head[group, place], h_rest[group, place]], axis=1),
            jnp.concatenate([table, table], axis=0),
            preferred_element_type=jnp.float32,
        )
        both = both[:, :TILE] + both[:, TILE:]
        real, imag = both[:TILE], both[TILE:]
        turn_real, turn_imag = turns[0, pl.ds(row_tile, 1), :], turns[1, pl.ds(row_tile, 1), :]
        return halves(
            jnp.concatenate(
                [real * turn_real - imag * turn_imag, real * turn_imag + imag * turn_real], axis=0
            )
        )

    def row_weights(spot, owner, place):
        for lane in range(0, samples, 128):
            position = asked[owner, place : place + 1, lane : lane + 128]
            cell = position // over
            inner = cell & 7
            value = look_up((row - inner) & 7, position)
            at = (cell // 8) + jnp.where(row < inner, 1, 0)
            parts = [part.astype(jnp.float32) for part in halves(value)]
            for pair in range(0, TILE // 8, 2):
                hits = [at == pair, at == pair + 1]
                for part, target in zip(parts, (rows_head, rows_rest)):
                    target[spot, pair * 8 : pair * 8 + 16, lane : lane + 128] = jnp.concatenate(
                        [jnp.where(hit, part, 0.0) for hit in hits], axis=0
                    ).astype(target.dtype)

    def predict(spot, owner, place):
        slot = spot % 2
        part = dot_exact(tile_head[slot], tile_rest[slot], rows_head[spot], rows_rest[spot])
        for lane in range(0, samples, 128):
            at = samples + lane
            position = asked[owner, place : place + 1, at : at + 128]
            cell = position // over
            column = []
            for j in range(0, tiles_across, 8):
                tap = (row + j - cell) & (tiles_across - 1)
                column.append(jnp.where(tap < support, look_up(tap, position), 0.0))
            away = row * tiles_across - cell
            sums = [jnp.zeros((8, 128), jnp.float32)] * 2
            for j in range(tiles_across):
                hit = ((away + j) & -tiles_across) == 0
                weight = jnp.where(hit, column[j // 8][j % 8 : j % 8 + 1], 0.0)
                for c in range(2):
                    cut = c * TILE + j * per
                    sums[c] = sums[c] + part[cut : cut + per, lane : lane + 128] * weight
            for c in range(2):
                at = c * samples + lane
                values[owner, place : place + 1, at : at + 128] = jnp.sum(sums[c], axis=0, keepdims=True)

    def answer(offset):
        index, where = peer(offset)
        return pltpu.make_async_remote_copy(
            src_ref=values.at[index],
            dst_ref=answers.at[me],
            send_sem=answer_send.at[offset],
            recv_sem=answer_recv.at[offset],
            device_id=where,
            device_id_type=pl.DeviceIdType.MESH,
        )

    steps = devices // unroll
    work_list = [(o + 1, c) for o in range(unroll) for c in range(capacity)]

    @pl.loop(0, steps)
    def _(step):
        begin = step * unroll

        @pl.when(step < steps - 1)
        def _():
            receive(begin + unroll + 1)

        for o in range(unroll):
            tile_copy(begin + o + 1).wait()

        owners = [peer(begin + o)[0] for o in range(unroll + 1)]
        tiles = [asked_tiles[owners[o], c, 0] for o, c in work_list]
        last = len(work_list) - 1
        for spot, (o, c) in enumerate(work_list):
            row_weights(spot, owners[o], c)
            pair = form_tile(tiles[spot])
            if spot:
                predict(spot - 1, owners[work_list[spot - 1][0]], work_list[spot - 1][1])
            else:
                predict(last, owners[0], capacity - 1)
            tile_head[spot % 2], tile_rest[spot % 2] = pair

        @pl.when(step > 0)
        def _():
            answer(begin).start()

        for o in range(1, unroll):
            answer(begin + o).start()

    predict(len(work_list) - 1, me, capacity - 1)
    answers[me] = values[me]

    @pl.loop(1, devices)
    def _(offset):
        request(offset).wait_send()
        answer(offset).wait()

    @pl.loop(0, blocks)
    def _(b):
        p = planes_ref[0, b]
        k = jnp.int32(0)
        for earlier in range(blocks):
            k = k + jnp.where((planes_ref[0, earlier] == p) & (earlier < b), 1, 0)
        total = answers[p * slabs]
        for a in range(1, slabs):
            total += answers[p * slabs + a]
        own = total[0:1]
        for place in range(1, capacity):
            own = jnp.where(k == place, total[place : place + 1], own)
        for c in range(2):
            out_ref[b, c : c + 1, :] = own[:, c * samples : (c + 1) * samples]


def shards(sky_model, plane_w, kernel, tile_ids, plane_ids, positions, observed):
    extent, columns = sky_model.shape[1:]
    planes, slabs = lax.axis_size("ba"), lax.axis_size("wa")
    devices = planes * slabs
    block_count, _, samples = positions.shape
    tiles_across = extent // TILE
    capacity = max(2, block_count // planes)
    smem = pl.BlockSpec(memory_space=pltpu.SMEM)
    vmem = pl.BlockSpec(memory_space=pltpu.VMEM)
    hbm = pl.BlockSpec(memory_space=pltpu.HBM)
    length = 2 * samples + 128

    lanes = columns // 2
    share = tiles_across * 8 // TILE
    unroll = math.gcd(devices, 4)
    over, support = kernel.shape
    y_head, y_rest = y_tables(extent)
    e_both = x_tables(extent, columns)
    basis = jnp.asarray(interpolation(16))
    half = jnp.bfloat16
    dma = pltpu.SemaphoreType.DMA
    predicted = pl.pallas_call(
        functools.partial(plane_kernel, extent, unroll),
        in_specs=[hbm, hbm, smem, hbm, hbm, hbm, hbm, hbm, hbm, hbm],
        out_specs=vmem,
        out_shape=pltpu.VMEM(observed.shape, jnp.float32),
        scratch_shapes=[
            pltpu.SMEM((1, block_count), jnp.int32),
            pltpu.SMEM((block_count,), jnp.int32),
            pltpu.SMEM((support, over), jnp.float32),
            pltpu.VMEM(positions.shape, jnp.int32),
            pltpu.VMEM(basis.shape, half),
            pltpu.VMEM((2, extent, columns), jnp.float32),
            pltpu.VMEM((tiles_across, TILE, 2 * lanes), jnp.float32),
            pltpu.VMEM((2, tiles_across, 2 * TILE, lanes), jnp.float32),
            pltpu.VMEM((tiles_across // share, share, 2 * TILE, columns), half),
            pltpu.VMEM((tiles_across // share, share, 2 * TILE, columns), half),
            pltpu.VMEM(y_head.shape, half),
            pltpu.VMEM(y_head.shape, half),
            pltpu.VMEM(e_both.shape, half),
            pltpu.VMEM((2, tiles_across, TILE), jnp.float32),
            pltpu.VMEM((unroll * capacity, TILE, samples), half),
            pltpu.VMEM((unroll * capacity, TILE, samples), half),
            pltpu.VMEM((2, 2 * TILE, TILE), half),
            pltpu.VMEM((2, 2 * TILE, TILE), half),
            pltpu.VMEM((planes, capacity, length), jnp.int32),
            pltpu.VMEM((devices, capacity, length), jnp.int32),
            pltpu.SMEM((devices, capacity, 128), jnp.int32),
            pltpu.VMEM((devices, capacity, 2 * samples), jnp.float32),
            pltpu.VMEM((devices, capacity, 2 * samples), jnp.float32),
            pltpu.VMEM((1, over * support), jnp.float32),
            dma((10,)),
            dma((devices,)),
            dma((devices,)),
            dma((devices,)),
            dma((devices,)),
            dma((devices,)),
        ],
        compiler_params=pltpu.CompilerParams(
            vmem_limit_bytes=62 << 20, collective_id=0, has_side_effects=True
        ),
        name="plane",
    )(
        plane_ids.T, tile_ids, plane_w, kernel.T, positions, sky_model, basis,
        jnp.asarray(y_head), jnp.asarray(y_rest), jnp.asarray(e_both),
    )
    return observed - predicted


def solution(mesh):
    return jax.shard_map(
        shards,
        mesh=mesh,
        in_specs=(
            P(None, None, "wa"),
            P("ba"),
            P(),
            P(("ba", "wa")),
            P(("ba", "wa"), None),
            P(("ba", "wa"), None, None),
            P(("ba", "wa"), None, None),
        ),
        out_specs=P(("ba", "wa"), None, None),
        check_vma=False,
    )
```

```python
import functools
import math

import jax
import jax.numpy as jnp
import numpy as np
from jax import lax
from jax.experimental import pallas as pl
from jax.experimental.pallas import tpu as pltpu
from jax.sharding import PartitionSpec as P

TILE = 128
FIELD_WIDTH = 0.7


def halves(values):
    head = values.astype(jnp.bfloat16)
    rest = (values - head.astype(jnp.float32)).astype(jnp.bfloat16)
    return head, rest


def host_halves(values):
    values = values.astype(np.float32)
    head = values.astype(jnp.bfloat16)
    rest = (values - head.astype(np.float32)).astype(jnp.bfloat16)
    return head, rest


def roots(index, modulus):
    angle = -2.0 * np.pi * (index % modulus) / modulus
    return np.cos(angle), np.sin(angle)


def y_tables(extent):
    panels = extent // TILE
    residue = np.arange(panels, dtype=np.int64)[:, None, None]
    step = np.arange(TILE, dtype=np.int64)[None, :, None]
    row = np.arange(TILE, dtype=np.int64)[None, None, :]
    real, imag = roots((panels * step + residue) * row, extent)
    table = np.concatenate(
        [np.concatenate([real, -imag], axis=2), np.concatenate([imag, real], axis=2)], axis=1
    )
    return host_halves(table)


def x_tables(extent, columns):
    tiles = np.arange(extent // TILE, dtype=np.int64)[:, None, None]
    pair = np.arange(columns // 2, dtype=np.int64)[None, :, None]
    cell = np.arange(TILE, dtype=np.int64)[None, None, :]
    real, imag = roots((tiles * TILE + cell) * (2 * pair + 1), 2 * extent)
    return np.concatenate(host_halves(np.concatenate([real, -imag], axis=1)), axis=2)


def fit(function, top, terms):
    nodes = (np.cos((np.arange(400) + 0.5) * np.pi / 400) + 1.0) * 0.5 * top
    series = np.polynomial.chebyshev.Chebyshev.fit(nodes, function(nodes), terms - 1, domain=[0, top])
    return [float(c) for c in series.convert(kind=np.polynomial.Polynomial).coef]


def horner(coefficients, argument):
    total = coefficients[-1]
    for coefficient in coefficients[-2::-1]:
        total = total * argument + coefficient
    return total


def small_dft(values):
    count = len(values)
    if count == 1:
        return [values[0]()]
    even = small_dft(values[0::2])
    odd = small_dft(values[1::2])
    low, high = [], []
    for k in range(count // 2):
        real, imag = odd[k]
        if k == 0:
            pass
        elif 4 * k == count:
            real, imag = imag, -real
        elif 8 * k == count:
            h = math.sqrt(0.5)
            real, imag = (real + imag) * h, (imag - real) * h
        elif 8 * k == 3 * count:
            h = math.sqrt(0.5)
            real, imag = (imag - real) * h, (real + imag) * -h
        else:
            c = math.cos(-2.0 * math.pi * k / count)
            s = math.sin(-2.0 * math.pi * k / count)
            real, imag = real * c - imag * s, real * s + imag * c
        low.append((even[k][0] + real, even[k][1] + imag))
        high.append((even[k][0] - real, even[k][1] - imag))
    return low + high


def lane_lookup(table, index):
    numbers = lax.GatherDimensionNumbers(
        offset_dims=(),
        collapsed_slice_dims=(1,),
        start_index_map=(1,),
        operand_batching_dims=(0,),
        start_indices_batching_dims=(0,),
    )
    return lax.gather(
        table, index[..., None], numbers, (1, 1), mode=lax.GatherScatterMode.PROMISE_IN_BOUNDS
    )


def dot_exact(head_a, rest_a, head_b, rest_b):
    return jnp.dot(
        jnp.concatenate([head_a, head_a, rest_a], axis=1),
        jnp.concatenate([head_b, rest_b, head_b], axis=0),
        preferred_element_type=jnp.float32,
    )


def interpolation(nodes):
    place = (np.arange(nodes) + 0.5) * np.pi / nodes
    at = np.arccos((np.arange(TILE) - (TILE - 1) / 2) / (TILE / 2))
    order = np.arange(nodes)
    scale = np.where(order == 0, 1.0, 2.0) / nodes
    head, rest = host_halves((np.cos(at[:, None] * order) * scale) @ np.cos(order[:, None] * place))
    return np.concatenate([head, head, rest], axis=1)


def y_phases(extent, first, stride, lanes, w, basis_ref, phases):
    panels = extent // TILE
    nodes = basis_ref.shape[1] // 3
    spacing = FIELD_WIDTH / extent
    edge = 2.0 * (FIELD_WIDTH / 2 * (1.0 + TILE / extent)) ** 2
    lower = fit(lambda r: 1.0 / (1.0 + np.sqrt(1.0 - r)), edge, 7)
    sine = fit(lambda z: np.sin(2 * np.pi * np.sqrt(z)) / np.sqrt(z), 0.25, 7)
    cosine = fit(lambda z: np.cos(2 * np.pi * np.sqrt(z)), 0.25, 7)
    x = lax.broadcasted_iota(jnp.int32, (nodes, lanes), 1) * stride + first
    x = (x.astype(jnp.float32) - extent / 2) * spacing
    x_sq = x * x
    node = lax.broadcasted_iota(jnp.int32, (nodes, 128), 0).astype(jnp.float32)
    node = jnp.cos((node + 0.5) * (math.pi / nodes)) * (TILE / 2) + (TILE - 1) / 2
    node = jnp.concatenate([node] * (lanes // 128), axis=1)
    basis = basis_ref[...]
    unroll = math.gcd(panels, 8)

    @pl.loop(0, panels // unroll)
    def _(step):
        for i in range(unroll):
            panel = step * unroll + i
            y = (node + ((panel * TILE).astype(jnp.float32) - extent / 2)) * spacing
            radius = x_sq + y * y
            turns = radius * horner(lower, radius) * w
            turns = turns - jnp.round(turns)
            square = turns * turns
            both = jnp.concatenate([horner(cosine, square), turns * horner(sine, square)], axis=1)
            head, rest = halves(both)
            phases[panel] = jnp.dot(
                basis, jnp.concatenate([head, rest, head], axis=0), preferred_element_type=jnp.float32
            )


def y_combine(extent, side, lanes, sky_ref, phases, work):
    panels = extent // TILE

    @pl.loop(0, TILE // 8, unroll=4)
    def _(group):
        base = pl.multiple_of(group * 8, 8)
        mirror = 127 - lax.broadcasted_iota(jnp.int32, (8, 128), 1)
        for lane in range(0, lanes, 128):
            at = lanes + lane if side else lanes - 128 - lane

            def value(panel):
                c = phases[panel, pl.ds(base, 8), pl.ds(lane, 128)]
                s = phases[panel, pl.ds(base, 8), pl.ds(lanes + lane, 128)]
                real, imag = (
                    sky_ref[part, pl.ds(base + panel * TILE, 8), pl.ds(at, 128)] for part in range(2)
                )
                if not side:
                    real, imag = lane_lookup(real, mirror), lane_lookup(imag, mirror)
                return real * c - imag * s, real * s + imag * c

            values = [functools.partial(value, panel) for panel in range(panels)]
            for residue, (real, imag) in enumerate(small_dft(values)):
                work[side, residue, pl.ds(base, 8), pl.ds(lane, 128)] = real
                work[side, residue, pl.ds(base + TILE, 8), pl.ds(lane, 128)] = imag


def y_finish(extent, work, table_head, table_rest, h_head, h_rest):
    panels = extent // TILE
    per_tile = TILE // panels
    share = 8 // per_tile
    together = 16 // per_tile
    unroll = math.gcd(panels // together, 4)

    @pl.loop(0, panels // together // unroll)
    def _(major):
        for minor in range(unroll):
            step = major * unroll + minor
            products = []
            for i in range(together):
                residue = together * step + i
                low, high = work[0, residue], work[1, residue]
                turned = jnp.concatenate([high[TILE:] - low[TILE:], low[:TILE] - high[:TILE]], axis=0)
                head, rest = halves(jnp.concatenate([low + high, turned], axis=1))
                products.append(dot_exact(table_head[residue], table_rest[residue], head, rest))
            for part in range(2):
                rows = slice(part * TILE, (part + 1) * TILE)
                grouped = [product[rows].reshape(TILE // 8, 8, -1) for product in products]
                at = pl.multiple_of(part * TILE + step * 16, 16)
                for place in range(share):
                    cut = slice(place * per_tile, (place + 1) * per_tile)
                    head, rest = halves(jnp.concatenate([group[:, cut] for group in grouped], axis=1))
                    h_head[:, place, pl.ds(at, 16), :] = head
                    h_rest[:, place, pl.ds(at, 16), :] = rest


def build_taps(taps_ref):
    support, over = taps_ref.shape
    lane = lax.broadcasted_iota(jnp.int32, (1, over * support), 1)
    table = jnp.zeros((1, over * support), jnp.float32)
    for o in range(over):
        for k in range(support):
            table = jnp.where(lane == k * over + (over - 1 - o), taps_ref[k, o], table)
    return table


def plane_kernel(
    extent, unroll,
    planes_hbm, tiles_hbm, w_ref, kernel_hbm, pos_hbm, sky_hbm, basis_hbm, y_head, y_rest, e_both,
    out_ref,
    planes_ref, tiles_ref, kernel_ref, pos_ref, basis_ref,
    sky, phases, work, h_head, h_rest, yh, yr, eb, turns, rows_head, rows_rest, tile_head, tile_rest,
    send, asked, asked_tiles, values, answers, taps,
    local_sems, request_send, request_recv, answer_send, answer_recv, tile_sems,
):
    tiles_across = extent // TILE
    columns = sky.shape[2]
    lanes = columns // 2
    share = h_head.shape[1]
    planes, slabs = lax.axis_size("ba"), lax.axis_size("wa")
    devices = planes * slabs
    plane, slab = lax.axis_index("ba"), lax.axis_index("wa")
    me = plane * slabs + slab
    blocks, _, samples = pos_ref.shape
    capacity = send.shape[1]
    support, over = kernel_ref.shape
    per = TILE // tiles_across

    loads = [
        pltpu.make_async_copy(
            sky_hbm.at[:, :, pl.ds(i * lanes, lanes)], sky.at[:, :, pl.ds(i * lanes, lanes)], local_sems.at[i]
        )
        for i in range(2)
    ]
    copies = [
        pltpu.make_async_copy(source, target, local_sems.at[2 + i])
        for i, (source, target) in enumerate(((y_head, yh), (y_rest, yr), (e_both, eb)))
    ]
    small = [
        pltpu.make_async_copy(source, target, local_sems.at[5 + i])
        for i, (source, target) in enumerate(
            (
                (basis_hbm, basis_ref), (planes_hbm, planes_ref), (tiles_hbm, tiles_ref),
                (kernel_hbm, kernel_ref), (pos_hbm, pos_ref),
            )
        )
    ]
    for copy in small + loads + copies:
        copy.start()

    def peer(offset):
        index = lax.rem(me + offset, devices)
        return index, {"ba": index // slabs, "wa": index % slabs}

    barrier = pltpu.get_barrier_semaphore()

    @pl.loop(1, devices)
    def _(offset):
        pl.semaphore_signal(
            barrier, inc=1, device_id=peer(offset)[1], device_id_type=pl.DeviceIdType.MESH
        )

    first = slab * columns + lanes
    small[0].wait()
    y_phases(extent, first - 1, -1, lanes, w_ref[0], basis_ref, phases)
    for copy in small[1:]:
        copy.wait()

    @pl.loop(0, planes)
    def _(p):
        count = jnp.int32(0)
        found = [jnp.int32(0)] * capacity
        for b in range(blocks):
            match = planes_ref[0, b] == p
            for c in range(capacity):
                found[c] = jnp.where(match & (count == c), b, found[c])
            count = count + jnp.where(match, 1, 0)
        for c in range(capacity):
            b = found[c]
            for axis in range(2):
                send[p, c : c + 1, axis * samples : (axis + 1) * samples] = pos_ref[b, axis : axis + 1, :]
            send[p, c : c + 1, 2 * samples :] = jnp.full((1, 128), tiles_ref[b], jnp.int32)

    taps[...] = build_taps(kernel_ref)
    cell = lax.broadcasted_iota(jnp.int32, (tiles_across, TILE), 0) * TILE
    cell = cell + lax.broadcasted_iota(jnp.int32, (tiles_across, TILE), 1)
    angle = (cell * (2 * columns * slab + columns - 1)) % (2 * extent)
    angle = angle.astype(jnp.float32) * (-math.pi / extent)
    turns[0] = jnp.cos(angle) * (1.0 / extent)
    turns[1] = jnp.sin(angle) * (1.0 / extent)

    def request(offset):
        index, where = peer(offset)
        return pltpu.make_async_remote_copy(
            src_ref=send.at[index // slabs],
            dst_ref=asked.at[me],
            send_sem=request_send.at[offset],
            recv_sem=request_recv.at[offset],
            device_id=where,
            device_id_type=pl.DeviceIdType.MESH,
        )

    def tile_copy(offset):
        owner = peer(offset)[0]
        return pltpu.make_async_copy(
            asked.at[owner, :, pl.ds(2 * samples, 128)], asked_tiles.at[owner], tile_sems.at[offset - 1]
        )

    def receive(first):
        for o in range(unroll):
            offset = first + o

            @pl.when(offset < devices)
            def _():
                request(devices - offset).wait_recv()

            tile_copy(offset).start()

    pl.semaphore_wait(barrier, devices - 1)

    @pl.loop(1, devices)
    def _(i):
        request(devices - i).start()

    loads[0].wait()
    y_combine(extent, 0, lanes, sky, phases, work)
    asked[me] = send[plane]
    last = rows_head.shape[0] - 1
    rows_head[last] = jnp.zeros(rows_head.shape[1:], rows_head.dtype)
    rows_rest[last] = jnp.zeros(rows_rest.shape[1:], rows_rest.dtype)
    tile_head[1] = jnp.zeros(tile_head.shape[1:], tile_head.dtype)
    tile_rest[1] = jnp.zeros(tile_rest.shape[1:], tile_rest.dtype)
    y_phases(extent, first, 1, lanes, w_ref[0], basis_ref, phases)
    loads[1].wait()
    y_combine(extent, 1, lanes, sky, phases, work)
    copies[0].wait()
    copies[1].wait()
    receive(1)
    y_finish(extent, work, yh, yr, h_head, h_rest)
    copies[2].wait()

    row = lax.broadcasted_iota(jnp.int32, (8, 128), 0)
    table = jnp.broadcast_to(taps[...], (8, 128))

    def look_up(tap, position):
        return lane_lookup(table, ((tap * over) | ((over - 1) - (position & (over - 1)))) & 127)

    def form_tile(tile):
        row_tile = tile // tiles_across
        col_tile = tile % tiles_across
        group, place = col_tile // share, col_tile % share
        table = eb[row_tile]
        both = jnp.dot(
            jnp.concatenate([h_head[group, place], h_rest[group, place]], axis=1),
            jnp.concatenate([table, table], axis=0),
            preferred_element_type=jnp.float32,
        )
        both = both[:, :TILE] + both[:, TILE:]
        real, imag = both[:TILE], both[TILE:]
        turn_real, turn_imag = turns[0, pl.ds(row_tile, 1), :], turns[1, pl.ds(row_tile, 1), :]
        return halves(
            jnp.concatenate(
                [real * turn_real - imag * turn_imag, real * turn_imag + imag * turn_real], axis=0
            )
        )

    def row_weights(spot, owner, place):
        for lane in range(0, samples, 128):
            position = asked[owner, place : place + 1, lane : lane + 128]
            cell = position // over
            inner = cell & 7
            value = look_up((row - inner) & 7, position)
            at = (cell // 8) + jnp.where(row < inner, 1, 0)
            parts = [part.astype(jnp.float32) for part in halves(value)]
            for pair in range(0, TILE // 8, 2):
                hits = [at == pair, at == pair + 1]
                for part, target in zip(parts, (rows_head, rows_rest)):
                    target[spot, pair * 8 : pair * 8 + 16, lane : lane + 128] = jnp.concatenate(
                        [jnp.where(hit, part, 0.0) for hit in hits], axis=0
                    ).astype(target.dtype)

    def predict(spot, owner, place):
        slot = spot % 2
        part = dot_exact(tile_head[slot], tile_rest[slot], rows_head[spot], rows_rest[spot])
        for lane in range(0, samples, 128):
            at = samples + lane
            position = asked[owner, place : place + 1, at : at + 128]
            cell = position // over
            column = []
            for j in range(0, tiles_across, 8):
                tap = (row + j - cell) & (tiles_across - 1)
                column.append(jnp.where(tap < support, look_up(tap, position), 0.0))
            away = row * tiles_across - cell
            sums = [jnp.zeros((8, 128), jnp.float32)] * 2
            for j in range(tiles_across):
                hit = ((away + j) & -tiles_across) == 0
                weight = jnp.where(hit, column[j // 8][j % 8 : j % 8 + 1], 0.0)
                for c in range(2):
                    cut = c * TILE + j * per
                    sums[c] = sums[c] + part[cut : cut + per, lane : lane + 128] * weight
            for c in range(2):
                at = c * samples + lane
                values[owner, place : place + 1, at : at + 128] = jnp.sum(sums[c], axis=0, keepdims=True)

    def answer(offset):
        index, where = peer(offset)
        return pltpu.make_async_remote_copy(
            src_ref=values.at[index],
            dst_ref=answers.at[me],
            send_sem=answer_send.at[offset],
            recv_sem=answer_recv.at[offset],
            device_id=where,
            device_id_type=pl.DeviceIdType.MESH,
        )

    steps = devices // unroll
    work_list = [(o + 1, c) for o in range(unroll) for c in range(capacity)]

    @pl.loop(0, steps)
    def _(step):
        begin = step * unroll

        @pl.when(step < steps - 1)
        def _():
            receive(begin + unroll + 1)

        for o in range(unroll):
            tile_copy(begin + o + 1).wait()

        owners = [peer(begin + o)[0] for o in range(unroll + 1)]
        tiles = [asked_tiles[owners[o], c, 0] for o, c in work_list]
        last = len(work_list) - 1
        for spot, (o, c) in enumerate(work_list):
            row_weights(spot, owners[o], c)
            pair = form_tile(tiles[spot])
            if spot:
                predict(spot - 1, owners[work_list[spot - 1][0]], work_list[spot - 1][1])
            else:
                predict(last, owners[0], capacity - 1)
            tile_head[spot % 2], tile_rest[spot % 2] = pair

        @pl.when(step > 0)
        def _():
            answer(begin).start()

        for o in range(1, unroll):
            answer(begin + o).start()

    predict(len(work_list) - 1, me, capacity - 1)
    answers[me] = values[me]

    @pl.loop(1, devices)
    def _(offset):
        request(offset).wait_send()
        answer(offset).wait()

    @pl.loop(0, blocks)
    def _(b):
        p = planes_ref[0, b]
        k = jnp.int32(0)
        for earlier in range(blocks):
            k = k + jnp.where((planes_ref[0, earlier] == p) & (earlier < b), 1, 0)
        total = answers[p * slabs]
        for a in range(1, slabs):
            total += answers[p * slabs + a]
        own = total[0:1]
        for place in range(1, capacity):
            own = jnp.where(k == place, total[place : place + 1], own)
        for c in range(2):
            out_ref[b, c : c + 1, :] = own[:, c * samples : (c + 1) * samples]


def shards(sky_model, plane_w, kernel, tile_ids, plane_ids, positions, observed):
    extent, columns = sky_model.shape[1:]
    planes, slabs = lax.axis_size("ba"), lax.axis_size("wa")
    devices = planes * slabs
    block_count, _, samples = positions.shape
    tiles_across = extent // TILE
    capacity = max(2, block_count // planes)
    smem = pl.BlockSpec(memory_space=pltpu.SMEM)
    vmem = pl.BlockSpec(memory_space=pltpu.VMEM)
    hbm = pl.BlockSpec(memory_space=pltpu.HBM)
    length = 2 * samples + 128

    lanes = columns // 2
    share = tiles_across * 8 // TILE
    unroll = math.gcd(devices, 4)
    over, support = kernel.shape
    y_head, y_rest = y_tables(extent)
    e_both = x_tables(extent, columns)
    basis = jnp.asarray(interpolation(16))
    half = jnp.bfloat16
    dma = pltpu.SemaphoreType.DMA
    predicted = pl.pallas_call(
        functools.partial(plane_kernel, extent, unroll),
        in_specs=[hbm, hbm, smem, hbm, hbm, hbm, hbm, hbm, hbm, hbm],
        out_specs=vmem,
        out_shape=pltpu.VMEM(observed.shape, jnp.float32),
        scratch_shapes=[
            pltpu.SMEM((1, block_count), jnp.int32),
            pltpu.SMEM((block_count,), jnp.int32),
            pltpu.SMEM((support, over), jnp.float32),
            pltpu.VMEM(positions.shape, jnp.int32),
            pltpu.VMEM(basis.shape, half),
            pltpu.VMEM((2, extent, columns), jnp.float32),
            pltpu.VMEM((tiles_across, TILE, 2 * lanes), jnp.float32),
            pltpu.VMEM((2, tiles_across, 2 * TILE, lanes), jnp.float32),
            pltpu.VMEM((tiles_across // share, share, 2 * TILE, columns), half),
            pltpu.VMEM((tiles_across // share, share, 2 * TILE, columns), half),
            pltpu.VMEM(y_head.shape, half),
            pltpu.VMEM(y_head.shape, half),
            pltpu.VMEM(e_both.shape, half),
            pltpu.VMEM((2, tiles_across, TILE), jnp.float32),
            pltpu.VMEM((unroll * capacity, TILE, samples), half),
            pltpu.VMEM((unroll * capacity, TILE, samples), half),
            pltpu.VMEM((2, 2 * TILE, TILE), half),
            pltpu.VMEM((2, 2 * TILE, TILE), half),
            pltpu.VMEM((planes, capacity, length), jnp.int32),
            pltpu.VMEM((devices, capacity, length), jnp.int32),
            pltpu.SMEM((devices, capacity, 128), jnp.int32),
            pltpu.VMEM((devices, capacity, 2 * samples), jnp.float32),
            pltpu.VMEM((devices, capacity, 2 * samples), jnp.float32),
            pltpu.VMEM((1, over * support), jnp.float32),
            dma((10,)),
            dma((devices,)),
            dma((devices,)),
            dma((devices,)),
            dma((devices,)),
            dma((devices,)),
        ],
        compiler_params=pltpu.CompilerParams(
            vmem_limit_bytes=62 << 20, collective_id=0, has_side_effects=True
        ),
        name="plane",
    )(
        plane_ids.T, tile_ids, plane_w, kernel.T, positions, sky_model, basis,
        jnp.asarray(y_head), jnp.asarray(y_rest), jnp.asarray(e_both),
    )
    return observed - predicted


def solution(mesh):
    return jax.shard_map(
        shards,
        mesh=mesh,
        in_specs=(
            P(None, None, "wa"),
            P("ba"),
            P(),
            P(("ba", "wa")),
            P(("ba", "wa"), None),
            P(("ba", "wa"), None, None),
            P(("ba", "wa"), None, None),
        ),
        out_specs=P(("ba", "wa"), None, None),
        check_vma=False,
    )
```
